128 devices in a mesh: grp: 4 (over z), seq: 32 (over x, y, core).
Axes of the slice: x: 4, y: 4, z: 4, core: 2. Of those that a mesh axis runs over, the one named last changes fastest.
Arguments:
- latent: bfloat16 [4, 4096, 32, 256], P('grp', 'seq'), may hold values from -6 to 6
- up_key: bfloat16 [4, 128, 256], replicated, may hold values from -0.5 to 0.5
- up_value: bfloat16 [4, 128, 256], replicated, may hold values from -0.5 to 0.5
- queries: bfloat16 [8, 64, 128], replicated, may hold values from -240 to 240, as said below
- lengths: int32 [8], replicated, may hold values from 1 to 16384
- block_dest: int32 [4096], replicated, may hold values from 0 to 127, as said below
Outputs:
- decode_latent: bfloat16 [128, 4, 32, 32, 256], P(('grp', 'seq'))
- attended: float32 [8, 8192], replicated
The draws below stay inside these ranges and needn't reach their ends.
Inputs may be any that keep to these rules, and one draw needn't show every extreme that they name: `block_dest`: each aligned run of 128 entries (the blocks of one seq index in the prefill layout) names every decode device exactly once. `queries`: the new token's query entries, real-valued.
All inputs are finite; a program needn't handle non-finite values.
Results may differ from the reference program's by a relative error of at most 0.001.
Values may be sent and summed in bfloat16 or wider, within the bound.
A program may use at most 64 MiB of HBM per device.

```python
import jax
import jax.numpy as jnp
from jax import lax

Q_HEADS = 64
KV_HEADS = 8
HEAD_DIM = 128
RANK = 128
BATCH = 8
BT = 32
GROUPS = 4
DESTS = 128
BLOCKS = 4096
S_MAX = 16384


def draw_queries(key, part):
    drawn = jnp.clip(jax.random.normal(key, (BATCH, Q_HEADS, HEAD_DIM), jnp.float32), -4.0, 4.0)
    return drawn.astype(jnp.bfloat16)


def draw_block_dest(key, part):
    shards = BLOCKS // DESTS
    subkeys = jax.random.split(jax.random.fold_in(key, 11), shards)
    orders = jax.vmap(lambda subkey: jax.random.permutation(subkey, DESTS))(subkeys)
    return orders.reshape(BLOCKS).astype(jnp.int32)


def place_ends(values, key, least, largest):
    place = [jax.random.randint(jax.random.fold_in(key, axis), (), 0, length) for axis, length in enumerate(values.shape)]
    main_axis = values.shape.index(max(values.shape))
    next_to = place[:main_axis] + [(place[main_axis] + 1) % values.shape[main_axis]] + place[main_axis + 1:]
    return values.at[tuple(place)].set(least).at[tuple(next_to)].set(largest)


def steps_of(stream_key, shape, cuts, smallest, high):
    loudness = 1.0
    for position, blocks in cuts:
        steps = jax.random.uniform(jax.random.fold_in(jax.random.fold_in(stream_key, 6), position), (blocks,), jnp.float32, smallest / len(cuts), high / len(cuts))
        loudness = loudness * jnp.repeat(jnp.exp(steps), shape[position] // blocks).reshape((-1,) + (1,) * (len(shape) - 1 - position))
    return loudness


def noise(key, extent, spread, bound, pieces=(), kind=jnp.bfloat16):
    entries = spread * jax.random.normal(key, extent, jnp.float32)
    if pieces:
        entries = entries * steps_of(key, extent, pieces, -0.22, 0.18)
    return jnp.clip(entries, -bound, bound).astype(kind)


def setup_inputs(seed: int = 0) -> dict:
    streams_of = jax.random.split(jax.random.key(seed), 7)
    latent = noise(streams_of[0], (GROUPS, BLOCKS, BT, 2 * RANK), 1.0, 6.0, ((0, 4), (1, 32)))
    up_key = noise(streams_of[1], (GROUPS, RANK, KV_HEADS // GROUPS * HEAD_DIM), RANK ** -0.5, 0.5)
    up_value = noise(streams_of[2], (GROUPS, RANK, KV_HEADS // GROUPS * HEAD_DIM), RANK ** -0.5, 0.5)
    queries = draw_queries(jax.random.fold_in(streams_of[6], 71), 0)
    lengths = place_ends(jax.random.randint(streams_of[4], (BATCH,), 1, S_MAX + 1), jax.random.fold_in(streams_of[4], 1), 1, S_MAX).astype(jnp.int32)
    block_dest = draw_block_dest(jax.random.fold_in(streams_of[6], 71), 0)
    return dict(latent=latent, up_key=up_key, up_value=up_value, queries=queries, lengths=lengths, block_dest=block_dest)


def reference(latent, up_key, up_value, queries, lengths, block_dest):
    shards = BLOCKS // DESTS
    table = block_dest.reshape(shards, DESTS)
    row_ids = jnp.broadcast_to(jnp.arange(shards, dtype=jnp.int32)[:, None], (shards, DESTS))
    col_ids = jnp.broadcast_to(jnp.arange(DESTS, dtype=jnp.int32)[None, :], (shards, DESTS))
    source_order = jnp.zeros((shards, DESTS), jnp.int32).at[row_ids, table].set(col_ids)
    global_ids = row_ids * DESTS + source_order
    picked = latent[:, global_ids.T]
    decode_latent = jnp.transpose(picked, (1, 0, 2, 3, 4))
    per_group = KV_HEADS // GROUPS
    per_kv = Q_HEADS // KV_HEADS
    scale = 1.0 / math_sqrt(HEAD_DIM)
    query_f = queries.astype(jnp.float32).reshape(BATCH, GROUPS, per_group, per_kv, HEAD_DIM)
    positions = jnp.arange(S_MAX, dtype=jnp.int32)
    valid = positions[None, :] < lengths[:, None]

    def one_group(index):
        lat = lax.dynamic_index_in_dim(latent, index, 0, keepdims=False).astype(jnp.float32)
        lat = lat.reshape(BATCH, S_MAX, 2 * RANK)
        key_map = lax.dynamic_index_in_dim(up_key, index, 0, keepdims=False).astype(jnp.float32)
        value_map = lax.dynamic_index_in_dim(up_value, index, 0, keepdims=False).astype(jnp.float32)
        keys = jnp.einsum('bsr,rc->bsc', lat[..., :RANK], key_map, precision=lax.Precision.HIGHEST)
        values = jnp.einsum('bsr,rc->bsc', lat[..., RANK:], value_map, precision=lax.Precision.HIGHEST)
        keys = keys.reshape(BATCH, S_MAX, per_group, HEAD_DIM)
        values = values.reshape(BATCH, S_MAX, per_group, HEAD_DIM)
        query_g = lax.dynamic_index_in_dim(query_f, index, 1, keepdims=False)
        scores = jnp.einsum('bkjd,bskd->bkjs', query_g, keys, precision=lax.Precision.HIGHEST) * scale
        live = valid[:, None, None, :]
        scores = jnp.where(live, scores, -1e+30)
        row_max = lax.optimization_barrier(jnp.max(scores, axis=-1, keepdims=True))
        weights = jnp.where(live, jnp.exp(scores - row_max), 0.0)
        totals = lax.optimization_barrier(jnp.sum(weights, axis=-1))
        summed = jnp.einsum('bkjs,bskd->bkjd', weights, values, precision=lax.Precision.HIGHEST)
        return summed / totals[..., None]
    outputs = lax.map(one_group, jnp.arange(GROUPS, dtype=jnp.int32))
    attended = jnp.transpose(outputs, (1, 0, 2, 3, 4)).reshape(BATCH, Q_HEADS * HEAD_DIM)
    return (decode_latent, attended)

def math_sqrt(value):
    return float(value) ** 0.5
```

```python
import functools
import random

import jax
import jax.numpy as jnp
from jax import lax
from jax.experimental import pallas as pl
from jax.experimental.pallas import tpu as pltpu
from jax.sharding import Mesh
from jax.sharding import PartitionSpec as P

AXES = ("grp", "seq_0", "seq_1", "seq_2")
SEQ = AXES[1:]
MESH = pl.DeviceIdType.MESH
F32 = jnp.float32
BF16 = jnp.bfloat16
LOG2E = 1.4426950408889634
NT = (((1,), (1,)), ((), ()))
NN = (((1,), (0,)), ((), ()))


def flow_order(sizes):
    nz, nx, ny, nc = sizes
    flows = [
        (dz, dx, dy, dc)
        for dz in range(nz)
        for dx in range(nx)
        for dy in range(ny)
        for dc in range(nc)
        if (dz, dx, dy, dc) != (0, 0, 0, 0)
    ]
    random.Random(1).shuffle(flows)
    return flows


def split3(x):
    hi = x.astype(BF16)
    rest = x - hi.astype(F32)
    mid = rest.astype(BF16)
    low = (rest - mid.astype(F32)).astype(BF16)
    return hi, mid, low


def split_dot(x, w, dims):
    n = x.shape[0]
    out = lax.dot_general(jnp.concatenate(split3(x), 0), w, dims, preferred_element_type=F32)
    return out[0:n] + out[n : 2 * n] + out[2 * n : 3 * n]


def exchange_kernel(
    sizes, first, second,
    latent, up_key, up_value, queries, lengths, block_dest,
    received, attended,
    lat, send, key_map, value_map, query, dest_row, order_v, order_s, length_s,
    scores, part_own, part_all, result, results,
    lat_sem, small_sem, order_sem, send_sem, recv_sem, part_send, part_recv,
    res_send, res_recv, relay_send, relay_recv,
):
    nz, nx, ny, nc = sizes
    z, x, y, c = [lax.axis_index(a) for a in AXES]
    shard = (x * ny + y) * nc + c
    me = z * (nx * ny * nc) + shard
    blocks, tokens = lat.shape[0], lat.shape[1]
    quads = shard % 4
    batch_id = shard // 4

    def peer(offset):
        dz, dx, dy, dc = offset
        return ((z + dz) % nz, (x + dx) % nx, (y + dy) % ny, (c + dc) % nc)

    def index_of(p):
        return ((p[0] * nx + p[1]) * ny + p[2]) * nc + p[3]

    flows = flow_order(sizes)
    barrier = pltpu.get_barrier_semaphore()
    for offset in flows:
        pl.semaphore_signal(barrier, 1, device_id=peer(offset), device_id_type=MESH)

    dest_copy = pltpu.make_async_copy(block_dest.at[pl.ds(shard, 1)], dest_row, small_sem.at[0])
    dest_copy.start()
    lat_copy = pltpu.make_async_copy(latent, lat, lat_sem)
    lat_copy.start()
    small = [
        pltpu.make_async_copy(up_key.at[z], key_map, small_sem.at[1]),
        pltpu.make_async_copy(up_value.at[z], value_map, small_sem.at[2]),
        pltpu.make_async_copy(queries.at[batch_id, pl.ds(pl.multiple_of(z * 16, 16), 16)], query, small_sem.at[3]),
        pltpu.make_async_copy(lengths, length_s, small_sem.at[4]),
    ]
    for copy in small:
        copy.start()

    dest_copy.wait()
    rows = lax.broadcasted_iota(jnp.int32, (blocks, blocks), 0)
    hot = jnp.where(rows == dest_row[...], 1.0, 0.0).astype(BF16)
    lanes = lax.broadcasted_iota(jnp.int32, (16, blocks), 1).astype(F32).astype(BF16)
    order = lax.dot_general(lanes, hot, NT, preferred_element_type=F32)[0:8].astype(jnp.int32)
    order_v[...] = jnp.clip(order, 0, blocks - 1)
    order_copy = pltpu.make_async_copy(order_v.at[pl.ds(0, 1)], order_s, order_sem)
    order_copy.start()
    order_copy.wait()
    lat_copy.wait()

    @pl.loop(0, blocks, unroll=8)
    def _(d):
        send[d] = lat[order_s[0, d]]

    received[me] = send[me]

    pl.semaphore_wait(barrier, len(flows))

    def send_blocks(some):
        for offset in some:
            p = peer(offset)
            pltpu.make_async_remote_copy(
                send.at[index_of(p)], received.at[me], send_sem, recv_sem, device_id=p, device_id_type=MESH
            ).start()

    send_blocks(flows[:first])

    for copy in small:
        copy.wait()
    head_dim = query.shape[1]
    rank = lat.shape[2] // 2
    q0 = lax.dot_general(query[...], key_map[:, 0:head_dim], NT, preferred_element_type=F32)
    q1 = lax.dot_general(query[...], key_map[:, head_dim : 2 * head_dim], NT, preferred_element_type=F32)
    scale = LOG2E / float(head_dim) ** 0.5
    q_parts = jnp.concatenate(split3(jnp.concatenate([q0[0:8], q1[8:16]], 0) * scale), 0)
    length = length_s[batch_id]
    start = quads * (blocks * tokens)
    chunk_blocks = 16
    width = chunk_blocks * tokens
    best = jnp.full((16, 128), -1e30, F32)
    for i in range(blocks // chunk_blocks):
        keys = lat[i * chunk_blocks : (i + 1) * chunk_blocks, :, 0:rank].reshape(width, rank)
        s3 = lax.dot_general(q_parts, keys, NT, preferred_element_type=F32)
        s = s3[0:16] + s3[16:32] + s3[32:48]
        position = start + i * width + lax.broadcasted_iota(jnp.int32, (16, width), 1)
        s = jnp.where(position < length, s, -1e30)
        scores[:, i * width : (i + 1) * width] = s
        for j in range(width // 128):
            best = jnp.maximum(best, s[:, j * 128 : (j + 1) * 128])
    top = jnp.max(best, axis=1, keepdims=True)
    total = jnp.zeros((16, 128), F32)
    acc = jnp.zeros((32, rank), F32)
    for i in range(blocks // chunk_blocks):
        s = scores[:, i * width : (i + 1) * width]
        position = start + i * width + lax.broadcasted_iota(jnp.int32, (16, width), 1)
        w = jnp.where(position < length, jnp.exp2(s - top), 0.0)
        for j in range(width // 128):
            total = total + w[:, j * 128 : (j + 1) * 128]
        hi = w.astype(BF16)
        low = (w - hi.astype(F32)).astype(BF16)
        vals = lat[i * chunk_blocks : (i + 1) * chunk_blocks, :, rank : 2 * rank].reshape(width, rank)
        acc = acc + lax.dot_general(jnp.concatenate([hi, low], 0), vals, NN, preferred_element_type=F32)
    part_own[0:16] = acc[0:16] + acc[16:32]
    part_own[16:32] = jnp.broadcast_to(top, (16, 128))
    part_own[32:48] = jnp.broadcast_to(jnp.sum(total, axis=1, keepdims=True), (16, 128))
    part_all[quads] = part_own[...]

    for k in range(1, 4):
        other_y = y + (k // 2) * (1 - 2 * (y % 2))
        other_c = (c + k % 2) % 2
        pltpu.make_async_remote_copy(
            part_own, part_all.at[quads], part_send, part_recv, device_id=(z, x, other_y, other_c), device_id_type=MESH
        ).start()

    send_blocks(flows[first:second])

    three = part_all.at[pl.ds(0, 3)]
    pltpu.make_async_copy(three, three, part_recv).wait()
    tops = [part_all[k, 16:32] for k in range(4)]
    top = jnp.maximum(jnp.maximum(tops[0], tops[1]), jnp.maximum(tops[2], tops[3]))
    total = jnp.zeros((16, 128), F32)
    acc = jnp.zeros((16, 128), F32)
    for k in range(4):
        factor = jnp.exp2(tops[k] - top)
        total = total + part_all[k, 32:48] * factor
        acc = acc + part_all[k, 0:16] * factor
    mean = acc / total
    r0 = split_dot(mean[0:8], value_map[:, 0:head_dim], NN)
    r1 = split_dot(mean[8:16], value_map[:, head_dim : 2 * head_dim], NN)
    result[0:8] = r0
    result[8:16] = r1

    half = y // 2
    slot = half * (nx * nz) + x * nz + z
    dest_y = (y + c * (2 * (y % 2) - 1) + ny) % ny
    for dx, dz in random.Random(2).sample([(i, j) for i in range(nx) for j in range(nz)], nx * nz):
        pltpu.make_async_remote_copy(
            result, results.at[slot], res_send, res_recv,
            device_id=((z + dz) % nz, (x + dx) % nx, dest_y, 1 - c), device_id_type=MESH,
        ).start()

    send_blocks(flows[second:])

    per_half = nx * nz
    mine = c * half + (1 - c) * (1 - half)
    got = results.at[pl.ds(mine * per_half, per_half)]
    pltpu.make_async_copy(got, got, res_recv).wait()
    relay = pltpu.make_async_remote_copy(
        got, got, relay_send, relay_recv, device_id=(z, x, y, 1 - c), device_id_type=MESH
    )
    relay.start()
    relay.wait()
    for j in range(2):
        for zz in range(nz):
            for h in range(16):
                for xx in range(nx):
                    col = (zz * 16 + h) * 128
                    row = 2 * xx + j
                    attended[row : row + 1, col : col + 128] = results[j * per_half + xx * nz + zz, h : h + 1]

    pltpu.make_async_copy(part_all.at[pl.ds(0, 3)], part_all.at[pl.ds(0, 3)], part_send).wait()
    sixteen = results.at[pl.ds(0, per_half)]
    pltpu.make_async_copy(sixteen, sixteen, res_send).wait()
    rest = received.at[pl.ds(0, len(flows))]
    pltpu.make_async_copy(rest, rest, send_sem).wait()
    pltpu.make_async_copy(rest, rest, recv_sem).wait()


def store_kernel(received, attended, out0, out1, sem):
    a = pltpu.make_async_copy(received, out0, sem.at[0])
    b = pltpu.make_async_copy(attended, out1, sem.at[1])
    a.start()
    b.start()
    a.wait()
    b.wait()


def body(latent, up_key, up_value, queries, lengths, block_dest):
    sizes = tuple(lax.axis_size(a) for a in AXES)
    groups, rank, width = up_key.shape
    blocks, tokens, both = latent.shape[1:]
    batch, heads, head_dim = queries.shape
    hbm = pl.BlockSpec(memory_space=pltpu.MemorySpace.HBM)
    vmem = pl.BlockSpec(memory_space=pltpu.MemorySpace.VMEM)
    dma = pltpu.SemaphoreType.DMA
    received, attended = pl.pallas_call(
        functools.partial(exchange_kernel, sizes, 50, 90),
        out_shape=(pltpu.VMEM((blocks, tokens, both), BF16), pltpu.VMEM((batch, heads * head_dim), F32)),
        in_specs=[hbm] * 6,
        out_specs=(vmem, vmem),
        scratch_shapes=[
            pltpu.VMEM((blocks, tokens, both), BF16),
            pltpu.VMEM((blocks, tokens, both), BF16),
            pltpu.VMEM((rank, width), BF16),
            pltpu.VMEM((rank, width), BF16),
            pltpu.VMEM((heads // groups, head_dim), BF16),
            pltpu.VMEM((1, blocks), jnp.int32),
            pltpu.VMEM((8, blocks), jnp.int32),
            pltpu.SMEM((1, blocks), jnp.int32),
            pltpu.SMEM((batch,), jnp.int32),
            pltpu.VMEM((16, blocks * tokens), F32),
            pltpu.VMEM((48, 128), F32),
            pltpu.VMEM((4, 48, 128), F32),
            pltpu.VMEM((16, 128), F32),
            pltpu.VMEM((groups * batch, 16, 128), F32),
            dma, dma((5,)), dma, dma, dma, dma, dma, dma, dma, dma, dma,
        ],
        compiler_params=pltpu.CompilerParams(collective_id=1, has_side_effects=True),
        name="exchange",
    )(latent[0], up_key, up_value, queries, lengths, block_dest.reshape(-1, blocks))
    decode_latent, attended = pl.pallas_call(
        store_kernel,
        out_shape=(
            jax.ShapeDtypeStruct((blocks, tokens, both), BF16),
            jax.ShapeDtypeStruct((batch, heads * head_dim), F32),
        ),
        in_specs=[vmem, vmem],
        out_specs=(hbm, hbm),
        scratch_shapes=[dma((2,))],
        name="store",
    )(*[pltpu.with_memory_space_constraint(a, pltpu.MemorySpace.VMEM) for a in (received, attended)])
    return decode_latent.reshape(1, groups, blocks // groups, tokens, both), attended


def solution(mesh):
    finer = Mesh(mesh.devices.reshape(mesh.shape["grp"], 4, 4, 2), AXES)
    in_specs = (P("grp", SEQ, None, None), P(), P(), P(), P(), P())
    out_specs = (P(AXES, None, None, None, None), P())
    return jax.shard_map(body, mesh=finer, in_specs=in_specs, out_specs=out_specs, check_vma=False)
```

```python
import functools
import random

import jax
import jax.numpy as jnp
from jax import lax
from jax.experimental import pallas as pl
from jax.experimental.pallas import tpu as pltpu
from jax.sharding import Mesh
from jax.sharding import PartitionSpec as P

AXES = ("grp", "seq_0", "seq_1", "seq_2")
SEQ = AXES[1:]
MESH = pl.DeviceIdType.MESH
F32 = jnp.float32
BF16 = jnp.bfloat16
LOG2E = 1.4426950408889634
NT = (((1,), (1,)), ((), ()))
NN = (((1,), (0,)), ((), ()))
SEED = 1


def flow_stages(sizes):
    nz, nx, ny, nc = sizes
    stages = [[], [], [], []]
    for dz in range(nz):
        for dx in range(nx):
            for dy in range(ny):
                for dc in range(nc):
                    stages[(dz > 0) + (dx > 0) + (dy > 0)].append((dz, dx, dy, dc))
    near = stages[0][1:] + stages[1]
    for k, stage in enumerate((near, stages[2], stages[3])):
        random.Random(SEED + k).shuffle(stage)
    return near, stages[2], stages[3]


def split3(x):
    hi = x.astype(BF16)
    rest = x - hi.astype(F32)
    mid = rest.astype(BF16)
    low = (rest - mid.astype(F32)).astype(BF16)
    return hi, mid, low


def split_dot(x, w, dims):
    n = x.shape[0]
    out = lax.dot_general(jnp.concatenate(split3(x), 0), w, dims, preferred_element_type=F32)
    return out[0:n] + out[n : 2 * n] + out[2 * n : 3 * n]


def exchange_kernel(
    sizes, first,
    latent, up_key, up_value, queries, lengths, block_dest,
    received, attended,
    lat, send, key_map, value_map, query, dest_row, order_v, order_s, length_s,
    scores, part_own, part_all, result, results,
    lat_sem, small_sem, order_sem, send_sem, recv_sem, part_send, part_recv,
    res_send, res_recv, relay_send, relay_recv, in_x, in_y, in_all,
):
    nz, nx, ny, nc = sizes
    z, x, y, c = [lax.axis_index(a) for a in AXES]
    shard = (x * ny + y) * nc + c
    me = z * (nx * ny * nc) + shard
    blocks, tokens = lat.shape[0], lat.shape[1]
    quads = shard % 4
    batch_id = shard // 4

    def peer(offset):
        dz, dx, dy, dc = offset
        return ((z + dz) % nz, (x + dx) % nx, (y + dy) % ny, (c + dc) % nc)

    def index_of(p):
        return ((p[0] * nx + p[1]) * ny + p[2]) * nc + p[3]

    near, planes, cube = flow_stages(sizes)
    rings = [[(dz, 0, 0, 0) for dz in range(1, nz)], [(0, dx, 0, 0) for dx in range(1, nx)], [(0, 0, dy, 0) for dy in range(1, ny)]]
    barrier = pltpu.get_barrier_semaphore()

    def tell(semaphore, offsets):
        for offset in offsets:
            pl.semaphore_signal(semaphore, 1, device_id=peer(offset), device_id_type=MESH)

    tell(barrier, near)

    dest_copy = pltpu.make_async_copy(block_dest.at[pl.ds(shard, 1)], dest_row, small_sem.at[0])
    dest_copy.start()
    lat_copy = pltpu.make_async_copy(latent, lat, lat_sem)
    lat_copy.start()
    small = [
        pltpu.make_async_copy(up_key.at[z], key_map, small_sem.at[1]),
        pltpu.make_async_copy(up_value.at[z], value_map, small_sem.at[2]),
        pltpu.make_async_copy(queries.at[batch_id, pl.ds(pl.multiple_of(z * 16, 16), 16)], query, small_sem.at[3]),
        pltpu.make_async_copy(lengths, length_s, small_sem.at[4]),
    ]
    for copy in small:
        copy.start()

    dest_copy.wait()
    rows = lax.broadcasted_iota(jnp.int32, (blocks, blocks), 0)
    hot = jnp.where(rows == dest_row[...], 1.0, 0.0).astype(BF16)
    lanes = lax.broadcasted_iota(jnp.int32, (16, blocks), 1).astype(F32).astype(BF16)
    order = lax.dot_general(lanes, hot, NT, preferred_element_type=F32)[0:8].astype(jnp.int32)
    order_v[...] = jnp.clip(order, 0, blocks - 1)
    order_copy = pltpu.make_async_copy(order_v.at[pl.ds(0, 1)], order_s, order_sem)
    order_copy.start()
    order_copy.wait()
    lat_copy.wait()

    @pl.loop(0, blocks, unroll=8)
    def _(d):
        send[d] = lat[order_s[0, d]]

    received[me] = send[me]

    def send_blocks(some):
        for offset in some:
            p = peer(offset)
            pltpu.make_async_remote_copy(
                send.at[index_of(p)], received.at[me], send_sem, recv_sem, device_id=p, device_id_type=MESH
            ).start()

    pl.semaphore_wait(barrier, len(near))
    tell(in_x, rings[1])
    tell(in_y, rings[2])
    send_blocks(near)

    for copy in small:
        copy.wait()
    head_dim = query.shape[1]
    rank = lat.shape[2] // 2
    q0 = lax.dot_general(query[...], key_map[:, 0:head_dim], NT, preferred_element_type=F32)
    q1 = lax.dot_general(query[...], key_map[:, head_dim : 2 * head_dim], NT, preferred_element_type=F32)
    scale = LOG2E / float(head_dim) ** 0.5
    q_parts = jnp.concatenate(split3(jnp.concatenate([q0[0:8], q1[8:16]], 0) * scale), 0)
    length = length_s[batch_id]
    start = quads * (blocks * tokens)
    chunk_blocks = 16
    width = chunk_blocks * tokens
    best = jnp.full((16, 128), -1e30, F32)
    for i in range(blocks // chunk_blocks):
        keys = lat[i * chunk_blocks : (i + 1) * chunk_blocks, :, 0:rank].reshape(width, rank)
        s3 = lax.dot_general(q_parts, keys, NT, preferred_element_type=F32)
        s = s3[0:16] + s3[16:32] + s3[32:48]
        position = start + i * width + lax.broadcasted_iota(jnp.int32, (16, width), 1)
        s = jnp.where(position < length, s, -1e30)
        scores[:, i * width : (i + 1) * width] = s
        for j in range(width // 128):
            best = jnp.maximum(best, s[:, j * 128 : (j + 1) * 128])
    top = jnp.max(best, axis=1, keepdims=True)
    total = jnp.zeros((16, 128), F32)
    acc = jnp.zeros((32, rank), F32)
    for i in range(blocks // chunk_blocks):
        s = scores[:, i * width : (i + 1) * width]
        position = start + i * width + lax.broadcasted_iota(jnp.int32, (16, width), 1)
        w = jnp.where(position < length, jnp.exp2(s - top), 0.0)
        for j in range(width // 128):
            total = total + w[:, j * 128 : (j + 1) * 128]
        hi = w.astype(BF16)
        low = (w - hi.astype(F32)).astype(BF16)
        vals = lat[i * chunk_blocks : (i + 1) * chunk_blocks, :, rank : 2 * rank].reshape(width, rank)
        acc = acc + lax.dot_general(jnp.concatenate([hi, low], 0), vals, NN, preferred_element_type=F32)
    part_own[0:16] = acc[0:16] + acc[16:32]
    part_own[16:32] = jnp.broadcast_to(top, (16, 128))
    part_own[32:48] = jnp.broadcast_to(jnp.sum(total, axis=1, keepdims=True), (16, 128))
    part_all[quads] = part_own[...]

    for k in range(1, 4):
        other_y = y + (k // 2) * (1 - 2 * (y % 2))
        other_c = (c + k % 2) % 2
        pltpu.make_async_remote_copy(
            part_own, part_all.at[quads], part_send, part_recv, device_id=(z, x, other_y, other_c), device_id_type=MESH
        ).start()

    pl.semaphore_wait(in_x, nx - 1)
    pl.semaphore_wait(in_y, ny - 1)
    tell(in_all, rings[1])
    send_blocks(planes)

    three = part_all.at[pl.ds(0, 3)]
    pltpu.make_async_copy(three, three, part_recv).wait()
    tops = [part_all[k, 16:32] for k in range(4)]
    top = jnp.maximum(jnp.maximum(tops[0], tops[1]), jnp.maximum(tops[2], tops[3]))
    total = jnp.zeros((16, 128), F32)
    acc = jnp.zeros((16, 128), F32)
    for k in range(4):
        factor = jnp.exp2(tops[k] - top)
        total = total + part_all[k, 32:48] * factor
        acc = acc + part_all[k, 0:16] * factor
    mean = acc / total
    r0 = split_dot(mean[0:8], value_map[:, 0:head_dim], NN)
    r1 = split_dot(mean[8:16], value_map[:, head_dim : 2 * head_dim], NN)
    result[0:8] = r0
    result[8:16] = r1

    pl.semaphore_wait(in_all, nx - 1)
    send_blocks(cube[:first])

    half = y // 2
    slot = half * (nx * nz) + x * nz + z
    dest_y = (y + c * (2 * (y % 2) - 1) + ny) % ny
    for dx, dz in random.Random(2).sample([(i, j) for i in range(nx) for j in range(nz)], nx * nz):
        pltpu.make_async_remote_copy(
            result, results.at[slot], res_send, res_recv,
            device_id=((z + dz) % nz, (x + dx) % nx, dest_y, 1 - c), device_id_type=MESH,
        ).start()

    send_blocks(cube[first:])

    per_half = nx * nz
    mine = c * half + (1 - c) * (1 - half)
    got = results.at[pl.ds(mine * per_half, per_half)]
    pltpu.make_async_copy(got, got, res_recv).wait()
    relay = pltpu.make_async_remote_copy(
        got, got, relay_send, relay_recv, device_id=(z, x, y, 1 - c), device_id_type=MESH
    )
    relay.start()
    relay.wait()
    for j in range(2):
        for zz in range(nz):
            for h in range(16):
                for xx in range(nx):
                    col = (zz * 16 + h) * 128
                    row = 2 * xx + j
                    attended[row : row + 1, col : col + 128] = results[j * per_half + xx * nz + zz, h : h + 1]

    pltpu.make_async_copy(part_all.at[pl.ds(0, 3)], part_all.at[pl.ds(0, 3)], part_send).wait()
    sixteen = results.at[pl.ds(0, per_half)]
    pltpu.make_async_copy(sixteen, sixteen, res_send).wait()
    rest = received.at[pl.ds(0, blocks - 1)]
    pltpu.make_async_copy(rest, rest, send_sem).wait()
    pltpu.make_async_copy(rest, rest, recv_sem).wait()


def store_kernel(received, attended, out0, out1, sem):
    a = pltpu.make_async_copy(received, out0, sem.at[0])
    b = pltpu.make_async_copy(attended, out1, sem.at[1])
    a.start()
    b.start()
    a.wait()
    b.wait()


def body(latent, up_key, up_value, queries, lengths, block_dest):
    sizes = tuple(lax.axis_size(a) for a in AXES)
    groups, rank, width = up_key.shape
    blocks, tokens, both = latent.shape[1:]
    batch, heads, head_dim = queries.shape
    hbm = pl.BlockSpec(memory_space=pltpu.MemorySpace.HBM)
    vmem = pl.BlockSpec(memory_space=pltpu.MemorySpace.VMEM)
    dma = pltpu.SemaphoreType.DMA
    received, attended = pl.pallas_call(
        functools.partial(exchange_kernel, sizes, 12),
        out_shape=(pltpu.VMEM((blocks, tokens, both), BF16), pltpu.VMEM((batch, heads * head_dim), F32)),
        in_specs=[hbm] * 6,
        out_specs=(vmem, vmem),
        scratch_shapes=[
            pltpu.VMEM((blocks, tokens, both), BF16),
            pltpu.VMEM((blocks, tokens, both), BF16),
            pltpu.VMEM((rank, width), BF16),
            pltpu.VMEM((rank, width), BF16),
            pltpu.VMEM((heads // groups, head_dim), BF16),
            pltpu.VMEM((1, blocks), jnp.int32),
            pltpu.VMEM((8, blocks), jnp.int32),
            pltpu.SMEM((1, blocks), jnp.int32),
            pltpu.SMEM((batch,), jnp.int32),
            pltpu.VMEM((16, blocks * tokens), F32),
            pltpu.VMEM((48, 128), F32),
            pltpu.VMEM((4, 48, 128), F32),
            pltpu.VMEM((16, 128), F32),
            pltpu.VMEM((groups * batch, 16, 128), F32),
            dma, dma((5,)), dma, dma, dma, dma, dma, dma, dma, dma, dma,
            pltpu.SemaphoreType.REGULAR, pltpu.SemaphoreType.REGULAR, pltpu.SemaphoreType.REGULAR,
        ],
        compiler_params=pltpu.CompilerParams(collective_id=1, has_side_effects=True),
        name="exchange",
    )(latent[0], up_key, up_value, queries, lengths, block_dest.reshape(-1, blocks))
    decode_latent, attended = pl.pallas_call(
        store_kernel,
        out_shape=(
            jax.ShapeDtypeStruct((blocks, tokens, both), BF16),
            jax.ShapeDtypeStruct((batch, heads * head_dim), F32),
        ),
        in_specs=[vmem, vmem],
        out_specs=(hbm, hbm),
        scratch_shapes=[dma((2,))],
        name="store",
    )(*[pltpu.with_memory_space_constraint(a, pltpu.MemorySpace.VMEM) for a in (received, attended)])
    return decode_latent.reshape(1, groups, blocks // groups, tokens, both), attended


def solution(mesh):
    finer = Mesh(mesh.devices.reshape(mesh.shape["grp"], 4, 4, 2), AXES)
    in_specs = (P("grp", SEQ, None, None), P(), P(), P(), P(), P())
    out_specs = (P(AXES, None, None, None, None), P())
    return jax.shard_map(body, mesh=finer, in_specs=in_specs, out_specs=out_specs, check_vma=False)
```

```python
import functools
import random

import jax
import jax.numpy as jnp
from jax import lax
from jax.experimental import pallas as pl
from jax.experimental.pallas import tpu as pltpu
from jax.sharding import Mesh
from jax.sharding import PartitionSpec as P

AXES = ("grp", "seq_0", "seq_1", "seq_2")
SEQ = AXES[1:]
MESH = pl.DeviceIdType.MESH
F32 = jnp.float32
BF16 = jnp.bfloat16
LOG2E = 1.4426950408889634
NT = (((1,), (1,)), ((), ()))
NN = (((1,), (0,)), ((), ()))
SEED = 7
EARLY = 36


def loads_of(flow):
    loads = []
    for steps in flow[:3]:
        loads += {0: [0, 0], 1: [1, 0], 2: [1, 1], 3: [0, 1]}[steps]
    return loads


def balanced(flows, total, seed):
    left = list(flows)
    random.Random(seed).shuffle(left)
    order = []
    while left:
        def uneven(flow):
            after = [a + b for a, b in zip(total, loads_of(flow))]
            mean = sum(after) / len(after)
            return sum((a - mean) ** 2 for a in after)

        best = min(left, key=uneven)
        left.remove(best)
        order.append(best)
        total[:] = [a + b for a, b in zip(total, loads_of(best))]
    return order


def flow_stages(sizes):
    nz, nx, ny, nc = sizes
    stages = [[], [], [], []]
    for dz in range(nz):
        for dx in range(nx):
            for dy in range(ny):
                for dc in range(nc):
                    stages[(dz > 0) + (dx > 0) + (dy > 0)].append((dz, dx, dy, dc))
    total = [0] * 6
    near = balanced(stages[0][1:] + stages[1], total, SEED)
    second = balanced(stages[2], total, SEED + 1)
    third = balanced(second[EARLY:] + stages[3], total, SEED + 2)
    return near, second[:EARLY], third


def split3(x):
    hi = x.astype(BF16)
    rest = x - hi.astype(F32)
    mid = rest.astype(BF16)
    low = (rest - mid.astype(F32)).astype(BF16)
    return hi, mid, low


def split_dot(x, w, dims):
    n = x.shape[0]
    out = lax.dot_general(jnp.concatenate(split3(x), 0), w, dims, preferred_element_type=F32)
    return out[0:n] + out[n : 2 * n] + out[2 * n : 3 * n]


def exchange_kernel(
    sizes,
    latent, up_key, up_value, queries, lengths, block_dest,
    received, attended,
    lat, send, key_map, value_map, query, dest_row, order_v, order_s, length_s,
    scores, part_own, part_all, result, results,
    lat_sem, small_sem, order_sem, send_sem, recv_sem, part_send, part_recv,
    res_send, res_recv, relay_send, relay_recv, in_x, in_y, in_all,
):
    nz, nx, ny, nc = sizes
    z, x, y, c = [lax.axis_index(a) for a in AXES]
    shard = (x * ny + y) * nc + c
    me = z * (nx * ny * nc) + shard
    blocks, tokens = lat.shape[0], lat.shape[1]
    quads = shard % 4
    batch_id = shard // 4

    def peer(offset):
        dz, dx, dy, dc = offset
        return ((z + dz) % nz, (x + dx) % nx, (y + dy) % ny, (c + dc) % nc)

    def index_of(p):
        return ((p[0] * nx + p[1]) * ny + p[2]) * nc + p[3]

    near, planes, cube = flow_stages(sizes)
    rings = [[(dz, 0, 0, 0) for dz in range(1, nz)], [(0, dx, 0, 0) for dx in range(1, nx)], [(0, 0, dy, 0) for dy in range(1, ny)]]
    barrier = pltpu.get_barrier_semaphore()

    def tell(semaphore, offsets):
        for offset in offsets:
            pl.semaphore_signal(semaphore, 1, device_id=peer(offset), device_id_type=MESH)


    dest_copy = pltpu.make_async_copy(block_dest.at[pl.ds(shard, 1)], dest_row, small_sem.at[0])
    dest_copy.start()
    lat_copy = pltpu.make_async_copy(latent, lat, lat_sem)
    piece = blocks // 8
    for k in range(8):
        part = pl.ds(k * piece, piece)
        pltpu.make_async_copy(latent.at[part], lat.at[part], lat_sem).start()
    small = [
        pltpu.make_async_copy(up_key.at[z], key_map, small_sem.at[1]),
        pltpu.make_async_copy(up_value.at[z], value_map, small_sem.at[2]),
        pltpu.make_async_copy(queries.at[batch_id, pl.ds(pl.multiple_of(z * 16, 16), 16)], query, small_sem.at[3]),
        pltpu.make_async_copy(lengths, length_s, small_sem.at[4]),
    ]
    for copy in small:
        copy.start()

    tell(barrier, near)

    dest_copy.wait()
    rows = lax.broadcasted_iota(jnp.int32, (blocks, blocks), 0)
    hot = jnp.where(rows == dest_row[...], 1.0, 0.0).astype(BF16)
    lanes = lax.broadcasted_iota(jnp.int32, (16, blocks), 1).astype(F32).astype(BF16)
    order = lax.dot_general(lanes, hot, NT, preferred_element_type=F32)[0:8].astype(jnp.int32)
    order_v[...] = jnp.clip(order, 0, blocks - 1)
    order_copy = pltpu.make_async_copy(order_v.at[pl.ds(0, 1)], order_s, order_sem)
    order_copy.start()

    pl.semaphore_wait(barrier, len(near))
    tell(in_x, rings[1])
    tell(in_y, rings[2])

    order_copy.wait()
    lat_copy.wait()

    @pl.loop(0, blocks, unroll=8)
    def _(d):
        send[d] = lat[order_s[0, d]]

    received[me] = send[me]

    def send_blocks(some):
        for offset in some:
            p = peer(offset)
            pltpu.make_async_remote_copy(
                send.at[index_of(p)], received.at[me], send_sem, recv_sem, device_id=p, device_id_type=MESH
            ).start()

    send_blocks(near)

    for copy in small:
        copy.wait()
    head_dim = query.shape[1]
    rank = lat.shape[2] // 2
    q0 = lax.dot_general(query[...], key_map[:, 0:head_dim], NT, preferred_element_type=F32)
    q1 = lax.dot_general(query[...], key_map[:, head_dim : 2 * head_dim], NT, preferred_element_type=F32)
    scale = LOG2E / float(head_dim) ** 0.5
    q_parts = jnp.concatenate(split3(jnp.concatenate([q0[0:8], q1[8:16]], 0) * scale), 0)
    length = length_s[batch_id]
    start = quads * (blocks * tokens)
    chunk_blocks = 16
    width = chunk_blocks * tokens
    best = jnp.full((16, 128), -1e30, F32)
    for i in range(blocks // chunk_blocks):
        keys = lat[i * chunk_blocks : (i + 1) * chunk_blocks, :, 0:rank].reshape(width, rank)
        s3 = lax.dot_general(q_parts, keys, NT, preferred_element_type=F32)
        s = s3[0:16] + s3[16:32] + s3[32:48]
        position = start + i * width + lax.broadcasted_iota(jnp.int32, (16, width), 1)
        s = jnp.where(position < length, s, -1e30)
        scores[:, i * width : (i + 1) * width] = s
        for j in range(width // 128):
            best = jnp.maximum(best, s[:, j * 128 : (j + 1) * 128])
    top = jnp.max(best, axis=1, keepdims=True)
    total = jnp.zeros((16, 128), F32)
    acc = jnp.zeros((32, rank), F32)
    for i in range(blocks // chunk_blocks):
        s = scores[:, i * width : (i + 1) * width]
        position = start + i * width + lax.broadcasted_iota(jnp.int32, (16, width), 1)
        w = jnp.where(position < length, jnp.exp2(s - top), 0.0)
        for j in range(width // 128):
            total = total + w[:, j * 128 : (j + 1) * 128]
        hi = w.astype(BF16)
        low = (w - hi.astype(F32)).astype(BF16)
        vals = lat[i * chunk_blocks : (i + 1) * chunk_blocks, :, rank : 2 * rank].reshape(width, rank)
        acc = acc + lax.dot_general(jnp.concatenate([hi, low], 0), vals, NN, preferred_element_type=F32)
    part_own[0:16] = acc[0:16] + acc[16:32]
    part_own[16:32] = jnp.broadcast_to(top, (16, 128))
    part_own[32:48] = jnp.broadcast_to(jnp.sum(total, axis=1, keepdims=True), (16, 128))
    part_all[quads] = part_own[...]

    for k in range(1, 4):
        other_y = y + (k // 2) * (1 - 2 * (y % 2))
        other_c = (c + k % 2) % 2
        pltpu.make_async_remote_copy(
            part_own, part_all.at[quads], part_send, part_recv, device_id=(z, x, other_y, other_c), device_id_type=MESH
        ).start()

    pl.semaphore_wait(in_x, nx - 1)
    pl.semaphore_wait(in_y, ny - 1)
    tell(in_all, rings[1])
    send_blocks(planes)

    pl.semaphore_wait(in_all, nx - 1)

    three = part_all.at[pl.ds(0, 3)]
    pltpu.make_async_copy(three, three, part_recv).wait()
    tops = [part_all[k, 16:32] for k in range(4)]
    top = jnp.maximum(jnp.maximum(tops[0], tops[1]), jnp.maximum(tops[2], tops[3]))
    total = jnp.zeros((16, 128), F32)
    acc = jnp.zeros((16, 128), F32)
    for k in range(4):
        factor = jnp.exp2(tops[k] - top)
        total = total + part_all[k, 32:48] * factor
        acc = acc + part_all[k, 0:16] * factor
    mean = acc / total
    r0 = split_dot(mean[0:8], value_map[:, 0:head_dim], NN)
    r1 = split_dot(mean[8:16], value_map[:, head_dim : 2 * head_dim], NN)
    result[0:8] = r0
    result[8:16] = r1

    half = y // 2
    slot = half * (nx * nz) + x * nz + z
    dest_y = (y + c * (2 * (y % 2) - 1) + ny) % ny
    for dx, dz in random.Random(2).sample([(i, j) for i in range(nx) for j in range(nz)], nx * nz):
        pltpu.make_async_remote_copy(
            result, results.at[slot], res_send, res_recv,
            device_id=((z + dz) % nz, (x + dx) % nx, dest_y, 1 - c), device_id_type=MESH,
        ).start()

    send_blocks(cube)

    per_half = nx * nz
    mine = c * half + (1 - c) * (1 - half)
    got = results.at[pl.ds(mine * per_half, per_half)]
    pltpu.make_async_copy(got, got, res_recv).wait()
    relay = pltpu.make_async_remote_copy(
        got, got, relay_send, relay_recv, device_id=(z, x, y, 1 - c), device_id_type=MESH
    )
    relay.start()
    relay.wait()
    for j in range(2):
        for zz in range(nz):
            for h in range(16):
                for xx in range(nx):
                    col = (zz * 16 + h) * 128
                    row = 2 * xx + j
                    attended[row : row + 1, col : col + 128] = results[j * per_half + xx * nz + zz, h : h + 1]

    pltpu.make_async_copy(part_all.at[pl.ds(0, 3)], part_all.at[pl.ds(0, 3)], part_send).wait()
    sixteen = results.at[pl.ds(0, per_half)]
    pltpu.make_async_copy(sixteen, sixteen, res_send).wait()
    rest = received.at[pl.ds(0, blocks - 1)]
    pltpu.make_async_copy(rest, rest, send_sem).wait()
    pltpu.make_async_copy(rest, rest, recv_sem).wait()


def store_kernel(received, attended, out0, out1, sem):
    copies = [
        pltpu.make_async_copy(received, out0, sem.at[0]),
        pltpu.make_async_copy(attended, out1, sem.at[1]),
    ]
    for copy in copies:
        copy.start()
    for copy in copies:
        copy.wait()


def body(latent, up_key, up_value, queries, lengths, block_dest):
    sizes = tuple(lax.axis_size(a) for a in AXES)
    groups, rank, width = up_key.shape
    blocks, tokens, both = latent.shape[1:]
    batch, heads, head_dim = queries.shape
    hbm = pl.BlockSpec(memory_space=pltpu.MemorySpace.HBM)
    vmem = pl.BlockSpec(memory_space=pltpu.MemorySpace.VMEM)
    dma = pltpu.SemaphoreType.DMA
    received, attended = pl.pallas_call(
        functools.partial(exchange_kernel, sizes),
        out_shape=(pltpu.VMEM((blocks, tokens, both), BF16), pltpu.VMEM((batch, heads * head_dim), F32)),
        in_specs=[hbm] * 6,
        out_specs=(vmem, vmem),
        scratch_shapes=[
            pltpu.VMEM((blocks, tokens, both), BF16),
            pltpu.VMEM((blocks, tokens, both), BF16),
            pltpu.VMEM((rank, width), BF16),
            pltpu.VMEM((rank, width), BF16),
            pltpu.VMEM((heads // groups, head_dim), BF16),
            pltpu.VMEM((1, blocks), jnp.int32),
            pltpu.VMEM((8, blocks), jnp.int32),
            pltpu.SMEM((1, blocks), jnp.int32),
            pltpu.SMEM((batch,), jnp.int32),
            pltpu.VMEM((16, blocks * tokens), F32),
            pltpu.VMEM((48, 128), F32),
            pltpu.VMEM((4, 48, 128), F32),
            pltpu.VMEM((16, 128), F32),
            pltpu.VMEM((groups * batch, 16, 128), F32),
            dma, dma((5,)), dma, dma, dma, dma, dma, dma, dma, dma, dma,
            pltpu.SemaphoreType.REGULAR, pltpu.SemaphoreType.REGULAR, pltpu.SemaphoreType.REGULAR,
        ],
        compiler_params=pltpu.CompilerParams(collective_id=1, has_side_effects=True),
        name="exchange",
    )(latent[0], up_key, up_value, queries, lengths, block_dest.reshape(-1, blocks))
    decode_latent, attended = pl.pallas_call(
        store_kernel,
        out_shape=(
            jax.ShapeDtypeStruct((blocks, tokens, both), BF16),
            jax.ShapeDtypeStruct((batch, heads * head_dim), F32),
        ),
        in_specs=[vmem, vmem],
        out_specs=(hbm, hbm),
        scratch_shapes=[dma((2,))],
        name="store",
    )(*[pltpu.with_memory_space_constraint(a, pltpu.MemorySpace.VMEM) for a in (received, attended)])
    return decode_latent.reshape(1, groups, blocks // groups, tokens, both), attended


def solution(mesh):
    finer = Mesh(mesh.devices.reshape(mesh.shape["grp"], 4, 4, 2), AXES)
    in_specs = (P("grp", SEQ, None, None), P(), P(), P(), P(), P())
    out_specs = (P(AXES, None, None, None, None), P())
    return jax.shard_map(body, mesh=finer, in_specs=in_specs, out_specs=out_specs, check_vma=False)
```

```python
import functools
import random

import jax
import jax.numpy as jnp
from jax import lax
from jax.experimental import pallas as pl
from jax.experimental.pallas import tpu as pltpu
from jax.sharding import Mesh
from jax.sharding import PartitionSpec as P

AXES = ("grp", "seq_0", "seq_1", "seq_2")
SEQ = AXES[1:]
MESH = pl.DeviceIdType.MESH
F32 = jnp.float32
BF16 = jnp.bfloat16
LOG2E = 1.4426950408889634
NT = (((1,), (1,)), ((), ()))
NN = (((1,), (0,)), ((), ()))
SEED = 3
EARLY = 36


def loads_of(flow):
    loads = []
    for steps in flow[:3]:
        loads += {0: [0, 0], 1: [1, 0], 2: [1, 1], 3: [0, 1]}[steps]
    return loads


def balanced(flows, total, seed):
    left = list(flows)
    random.Random(seed).shuffle(left)
    order = []
    while left:
        def uneven(flow):
            after = [a + b for a, b in zip(total, loads_of(flow))]
            mean = sum(after) / len(after)
            return sum((a - mean) ** 2 for a in after)

        best = min(left, key=uneven)
        left.remove(best)
        order.append(best)
        total[:] = [a + b for a, b in zip(total, loads_of(best))]
    return order


def flow_stages(sizes):
    nz, nx, ny, nc = sizes
    stages = [[], [], [], []]
    for dz in range(nz):
        for dx in range(nx):
            for dy in range(ny):
                for dc in range(nc):
                    stages[(dz > 0) + (dx > 0) + (dy > 0)].append((dz, dx, dy, dc))
    total = [0] * 6
    near = balanced(stages[0][1:] + stages[1], total, SEED)
    second = balanced(stages[2], total, SEED + 1)
    third = balanced(second[EARLY:] + stages[3], total, SEED + 2)
    return near, second[:EARLY], third


def split3(x):
    hi = x.astype(BF16)
    rest = x - hi.astype(F32)
    mid = rest.astype(BF16)
    low = (rest - mid.astype(F32)).astype(BF16)
    return hi, mid, low


def split_dot(x, w, dims):
    n = x.shape[0]
    out = lax.dot_general(jnp.concatenate(split3(x), 0), w, dims, preferred_element_type=F32)
    return out[0:n] + out[n : 2 * n] + out[2 * n : 3 * n]


def exchange_kernel(
    sizes,
    latent, up_key, up_value, queries, lengths, block_dest,
    received, attended,
    lat, send, key_map, value_map, query, dest_row, order_v, order_s, length_s,
    scores, part_own, part_all, result, results,
    lat_sem, small_sem, order_sem, send_sem, recv_sem, part_send, part_recv,
    res_send, res_recv, relay_send, relay_recv, in_x, in_y, in_all,
):
    nz, nx, ny, nc = sizes
    z, x, y, c = [lax.axis_index(a) for a in AXES]
    shard = (x * ny + y) * nc + c
    me = z * (nx * ny * nc) + shard
    blocks, tokens = lat.shape[0], lat.shape[1]
    quads = shard % 4
    batch_id = shard // 4

    def peer(offset):
        dz, dx, dy, dc = offset
        return ((z + dz) % nz, (x + dx) % nx, (y + dy) % ny, (c + dc) % nc)

    def index_of(p):
        return ((p[0] * nx + p[1]) * ny + p[2]) * nc + p[3]

    near, planes, cube = flow_stages(sizes)
    rings = [[(dz, 0, 0, 0) for dz in range(1, nz)], [(0, dx, 0, 0) for dx in range(1, nx)], [(0, 0, dy, 0) for dy in range(1, ny)]]
    barrier = pltpu.get_barrier_semaphore()

    def tell(semaphore, offsets):
        for offset in offsets:
            pl.semaphore_signal(semaphore, 1, device_id=peer(offset), device_id_type=MESH)


    dest_copy = pltpu.make_async_copy(block_dest.at[pl.ds(shard, 1)], dest_row, small_sem.at[0])
    dest_copy.start()
    lat_copy = pltpu.make_async_copy(latent, lat, lat_sem)
    piece = blocks // 8
    for k in range(8):
        part = pl.ds(k * piece, piece)
        pltpu.make_async_copy(latent.at[part], lat.at[part], lat_sem).start()
    small = [
        pltpu.make_async_copy(up_key.at[z], key_map, small_sem.at[1]),
        pltpu.make_async_copy(up_value.at[z], value_map, small_sem.at[2]),
        pltpu.make_async_copy(queries.at[batch_id, pl.ds(pl.multiple_of(z * 16, 16), 16)], query, small_sem.at[3]),
        pltpu.make_async_copy(lengths, length_s, small_sem.at[4]),
    ]
    for copy in small:
        copy.start()

    tell(barrier, near)

    dest_copy.wait()
    rows = lax.broadcasted_iota(jnp.int32, (blocks, blocks), 0)
    hot = jnp.where(rows == dest_row[...], 1.0, 0.0).astype(BF16)
    lanes = lax.broadcasted_iota(jnp.int32, (16, blocks), 1).astype(F32).astype(BF16)
    order = lax.dot_general(lanes, hot, NT, preferred_element_type=F32)[0:8].astype(jnp.int32)
    order_v[...] = jnp.clip(order, 0, blocks - 1)
    order_copy = pltpu.make_async_copy(order_v.at[pl.ds(0, 1)], order_s, order_sem)
    order_copy.start()

    order_copy.wait()
    lat_copy.wait()

    @pl.loop(0, blocks, unroll=8)
    def _(d):
        send[d] = lat[order_s[0, d]]

    received[me] = send[me]

    turn = 1 - 2 * c

    def send_blocks(some):
        for dz, dx, dy, dc in some:
            p = peer((turn * dz + nz, turn * dx + nx, turn * dy + ny, dc))
            pltpu.make_async_remote_copy(
                send.at[index_of(p)], received.at[me], send_sem, recv_sem, device_id=p, device_id_type=MESH
            ).start()

    pl.semaphore_wait(barrier, len(near))
    tell(in_x, rings[1])
    tell(in_y, rings[2])
    send_blocks(near)

    for copy in small:
        copy.wait()
    head_dim = query.shape[1]
    rank = lat.shape[2] // 2
    q0 = lax.dot_general(query[...], key_map[:, 0:head_dim], NT, preferred_element_type=F32)
    q1 = lax.dot_general(query[...], key_map[:, head_dim : 2 * head_dim], NT, preferred_element_type=F32)
    scale = LOG2E / float(head_dim) ** 0.5
    q_parts = jnp.concatenate(split3(jnp.concatenate([q0[0:8], q1[8:16]], 0) * scale), 0)
    length = length_s[batch_id]
    start = quads * (blocks * tokens)
    chunk_blocks = 16
    width = chunk_blocks * tokens
    best = jnp.full((16, 128), -1e30, F32)
    for i in range(blocks // chunk_blocks):
        keys = lat[i * chunk_blocks : (i + 1) * chunk_blocks, :, 0:rank].reshape(width, rank)
        s3 = lax.dot_general(q_parts, keys, NT, preferred_element_type=F32)
        s = s3[0:16] + s3[16:32] + s3[32:48]
        position = start + i * width + lax.broadcasted_iota(jnp.int32, (16, width), 1)
        s = jnp.where(position < length, s, -1e30)
        scores[:, i * width : (i + 1) * width] = s
        for j in range(width // 128):
            best = jnp.maximum(best, s[:, j * 128 : (j + 1) * 128])
    top = jnp.max(best, axis=1, keepdims=True)
    total = jnp.zeros((16, 128), F32)
    acc = jnp.zeros((32, rank), F32)
    for i in range(blocks // chunk_blocks):
        s = scores[:, i * width : (i + 1) * width]
        position = start + i * width + lax.broadcasted_iota(jnp.int32, (16, width), 1)
        w = jnp.where(position < length, jnp.exp2(s - top), 0.0)
        for j in range(width // 128):
            total = total + w[:, j * 128 : (j + 1) * 128]
        hi = w.astype(BF16)
        low = (w - hi.astype(F32)).astype(BF16)
        vals = lat[i * chunk_blocks : (i + 1) * chunk_blocks, :, rank : 2 * rank].reshape(width, rank)
        acc = acc + lax.dot_general(jnp.concatenate([hi, low], 0), vals, NN, preferred_element_type=F32)
    part_own[0:16] = acc[0:16] + acc[16:32]
    part_own[16:32] = jnp.broadcast_to(top, (16, 128))
    part_own[32:48] = jnp.broadcast_to(jnp.sum(total, axis=1, keepdims=True), (16, 128))
    part_all[quads] = part_own[...]

    pl.semaphore_wait(in_x, nx - 1)
    pl.semaphore_wait(in_y, ny - 1)
    tell(in_all, rings[1])

    for k in range(1, 4):
        other_y = y + (k // 2) * (1 - 2 * (y % 2))
        other_c = (c + k % 2) % 2
        pltpu.make_async_remote_copy(
            part_own, part_all.at[quads], part_send, part_recv, device_id=(z, x, other_y, other_c), device_id_type=MESH
        ).start()

    send_blocks(planes)

    pl.semaphore_wait(in_all, nx - 1)

    three = part_all.at[pl.ds(0, 3)]
    pltpu.make_async_copy(three, three, part_recv).wait()
    tops = [part_all[k, 16:32] for k in range(4)]
    top = jnp.maximum(jnp.maximum(tops[0], tops[1]), jnp.maximum(tops[2], tops[3]))
    total = jnp.zeros((16, 128), F32)
    acc = jnp.zeros((16, 128), F32)
    for k in range(4):
        factor = jnp.exp2(tops[k] - top)
        total = total + part_all[k, 32:48] * factor
        acc = acc + part_all[k, 0:16] * factor
    mean = acc / total
    r0 = split_dot(mean[0:8], value_map[:, 0:head_dim], NN)
    r1 = split_dot(mean[8:16], value_map[:, head_dim : 2 * head_dim], NN)
    result[0:8] = r0
    result[8:16] = r1

    send_blocks(cube[:6])

    half = y // 2
    slot = half * (nx * nz) + x * nz + z
    dest_y = (y + c * (2 * (y % 2) - 1) + ny) % ny
    for dx, dz in random.Random(2).sample([(i, j) for i in range(nx) for j in range(nz)], nx * nz):
        pltpu.make_async_remote_copy(
            result, results.at[slot], res_send, res_recv,
            device_id=((z + dz) % nz, (x + dx) % nx, dest_y, 1 - c), device_id_type=MESH,
        ).start()

    send_blocks(cube[6:])

    per_half = nx * nz
    mine = c * half + (1 - c) * (1 - half)
    got = results.at[pl.ds(mine * per_half, per_half)]
    pltpu.make_async_copy(got, got, res_recv).wait()
    relay = pltpu.make_async_remote_copy(
        got, got, relay_send, relay_recv, device_id=(z, x, y, 1 - c), device_id_type=MESH
    )
    relay.start()
    relay.wait()
    for j in range(2):
        for zz in range(nz):
            for h in range(16):
                for xx in range(nx):
                    col = (zz * 16 + h) * 128
                    row = 2 * xx + j
                    attended[row : row + 1, col : col + 128] = results[j * per_half + xx * nz + zz, h : h + 1]

    pltpu.make_async_copy(part_all.at[pl.ds(0, 3)], part_all.at[pl.ds(0, 3)], part_send).wait()
    sixteen = results.at[pl.ds(0, per_half)]
    pltpu.make_async_copy(sixteen, sixteen, res_send).wait()
    rest = received.at[pl.ds(0, blocks - 1)]
    pltpu.make_async_copy(rest, rest, send_sem).wait()
    pltpu.make_async_copy(rest, rest, recv_sem).wait()


def store_kernel(received, attended, out0, out1, sem):
    copies = [
        pltpu.make_async_copy(received, out0, sem.at[0]),
        pltpu.make_async_copy(attended, out1, sem.at[1]),
    ]
    for copy in copies:
        copy.start()
    for copy in copies:
        copy.wait()


def body(latent, up_key, up_value, queries, lengths, block_dest):
    sizes = tuple(lax.axis_size(a) for a in AXES)
    groups, rank, width = up_key.shape
    blocks, tokens, both = latent.shape[1:]
    batch, heads, head_dim = queries.shape
    hbm = pl.BlockSpec(memory_space=pltpu.MemorySpace.HBM)
    vmem = pl.BlockSpec(memory_space=pltpu.MemorySpace.VMEM)
    dma = pltpu.SemaphoreType.DMA
    received, attended = pl.pallas_call(
        functools.partial(exchange_kernel, sizes),
        out_shape=(pltpu.VMEM((blocks, tokens, both), BF16), pltpu.VMEM((batch, heads * head_dim), F32)),
        in_specs=[hbm] * 6,
        out_specs=(vmem, vmem),
        scratch_shapes=[
            pltpu.VMEM((blocks, tokens, both), BF16),
            pltpu.VMEM((blocks, tokens, both), BF16),
            pltpu.VMEM((rank, width), BF16),
            pltpu.VMEM((rank, width), BF16),
            pltpu.VMEM((heads // groups, head_dim), BF16),
            pltpu.VMEM((1, blocks), jnp.int32),
            pltpu.VMEM((8, blocks), jnp.int32),
            pltpu.SMEM((1, blocks), jnp.int32),
            pltpu.SMEM((batch,), jnp.int32),
            pltpu.VMEM((16, blocks * tokens), F32),
            pltpu.VMEM((48, 128), F32),
            pltpu.VMEM((4, 48, 128), F32),
            pltpu.VMEM((16, 128), F32),
            pltpu.VMEM((groups * batch, 16, 128), F32),
            dma, dma((5,)), dma, dma, dma, dma, dma, dma, dma, dma, dma,
            pltpu.SemaphoreType.REGULAR, pltpu.SemaphoreType.REGULAR, pltpu.SemaphoreType.REGULAR,
        ],
        compiler_params=pltpu.CompilerParams(collective_id=1, has_side_effects=True),
        name="exchange",
    )(latent[0], up_key, up_value, queries, lengths, block_dest.reshape(-1, blocks))
    decode_latent, attended = pl.pallas_call(
        store_kernel,
        out_shape=(
            jax.ShapeDtypeStruct((blocks, tokens, both), BF16),
            jax.ShapeDtypeStruct((batch, heads * head_dim), F32),
        ),
        in_specs=[vmem, vmem],
        out_specs=(hbm, hbm),
        scratch_shapes=[dma((2,))],
        name="store",
    )(*[pltpu.with_memory_space_constraint(a, pltpu.MemorySpace.VMEM) for a in (received, attended)])
    return decode_latent.reshape(1, groups, blocks // groups, tokens, both), attended


def solution(mesh):
    finer = Mesh(mesh.devices.reshape(mesh.shape["grp"], 4, 4, 2), AXES)
    in_specs = (P("grp", SEQ, None, None), P(), P(), P(), P(), P())
    out_specs = (P(AXES, None, None, None, None), P())
    return jax.shard_map(body, mesh=finer, in_specs=in_specs, out_specs=out_specs, check_vma=False)
```

```python
import functools
import random

import jax
import jax.numpy as jnp
from jax import lax
from jax.experimental import pallas as pl
from jax.experimental.pallas import tpu as pltpu
from jax.sharding import Mesh
from jax.sharding import PartitionSpec as P

AXES = ("grp", "seq_0", "seq_1", "seq_2")
SEQ = AXES[1:]
MESH = pl.DeviceIdType.MESH
F32 = jnp.float32
BF16 = jnp.bfloat16
LOG2E = 1.4426950408889634
NT = (((1,), (1,)), ((), ()))
NN = (((1,), (0,)), ((), ()))
SEED = 3
EARLY = 36


def loads_of(flow):
    loads = []
    for steps in flow[:3]:
        loads += {0: [0, 0], 1: [1, 0], 2: [1, 1], 3: [0, 1]}[steps]
    return loads


def balanced(flows, total, seed):
    left = list(flows)
    random.Random(seed).shuffle(left)
    order = []
    while left:
        def uneven(flow):
            after = [a + b for a, b in zip(total, loads_of(flow))]
            mean = sum(after) / len(after)
            return sum((a - mean) ** 2 for a in after)

        best = min(left, key=uneven)
        left.remove(best)
        order.append(best)
        total[:] = [a + b for a, b in zip(total, loads_of(best))]
    return order


def flow_stages(sizes):
    nz, nx, ny, nc = sizes
    stages = [[], [], [], []]
    for dz in range(nz):
        for dx in range(nx):
            for dy in range(ny):
                for dc in range(nc):
                    stages[(dz > 0) + (dx > 0) + (dy > 0)].append((dz, dx, dy, dc))
    total = [0] * 6
    near = balanced(stages[0][1:] + stages[1], total, SEED)
    second = balanced(stages[2], total, SEED + 1)
    third = balanced(second[EARLY:] + stages[3], total, SEED + 2)
    return near, second[:EARLY], third


def split3(x):
    hi = x.astype(BF16)
    rest = x - hi.astype(F32)
    mid = rest.astype(BF16)
    low = (rest - mid.astype(F32)).astype(BF16)
    return hi, mid, low


def split_dot(x, w, dims):
    n = x.shape[0]
    out = lax.dot_general(jnp.concatenate(split3(x), 0), w, dims, preferred_element_type=F32)
    return out[0:n] + out[n : 2 * n] + out[2 * n : 3 * n]


def exchange_kernel(
    sizes,
    latent, up_key, up_value, queries, lengths, block_dest,
    received, attended,
    lat, send, key_map, value_map, query, dest_row, order_v, order_s, length_s,
    scores, part_own, part_all, result, results,
    lat_sem, small_sem, order_sem, send_sem, recv_sem, part_send, part_recv,
    res_send, res_recv, relay_send, relay_recv, in_x, in_y, in_all,
):
    nz, nx, ny, nc = sizes
    z, x, y, c = [lax.axis_index(a) for a in AXES]
    shard = (x * ny + y) * nc + c
    me = z * (nx * ny * nc) + shard
    blocks, tokens = lat.shape[0], lat.shape[1]
    quads = shard % 4
    batch_id = shard // 4

    def peer(offset):
        dz, dx, dy, dc = offset
        return ((z + dz) % nz, (x + dx) % nx, (y + dy) % ny, (c + dc) % nc)

    def index_of(p):
        return ((p[0] * nx + p[1]) * ny + p[2]) * nc + p[3]

    near, planes, cube = flow_stages(sizes)
    rings = [[(dz, 0, 0, 0) for dz in range(1, nz)], [(0, dx, 0, 0) for dx in range(1, nx)], [(0, 0, dy, 0) for dy in range(1, ny)]]
    barrier = pltpu.get_barrier_semaphore()

    def tell(semaphore, offsets):
        for offset in offsets:
            pl.semaphore_signal(semaphore, 1, device_id=peer(offset), device_id_type=MESH)


    dest_copy = pltpu.make_async_copy(block_dest.at[pl.ds(shard, 1)], dest_row, small_sem.at[0])
    dest_copy.start()
    lat_copy = pltpu.make_async_copy(latent, lat, lat_sem)
    piece = blocks // 32
    for k in range(32):
        part = pl.ds(k * piece, piece)
        pltpu.make_async_copy(latent.at[part], lat.at[part], lat_sem).start()
    small = [
        pltpu.make_async_copy(up_key.at[z], key_map, small_sem.at[1]),
        pltpu.make_async_copy(up_value.at[z], value_map, small_sem.at[2]),
        pltpu.make_async_copy(queries.at[batch_id, pl.ds(pl.multiple_of(z * 16, 16), 16)], query, small_sem.at[3]),
        pltpu.make_async_copy(lengths, length_s, small_sem.at[4]),
    ]
    for copy in small:
        copy.start()

    tell(barrier, near)

    dest_copy.wait()
    rows = lax.broadcasted_iota(jnp.int32, (blocks, blocks), 0)
    hot = jnp.where(rows == dest_row[...], 1.0, 0.0).astype(BF16)
    lanes = lax.broadcasted_iota(jnp.int32, (16, blocks), 1).astype(F32).astype(BF16)
    order = lax.dot_general(lanes, hot, NT, preferred_element_type=F32)[0:8].astype(jnp.int32)
    order_v[...] = jnp.clip(order, 0, blocks - 1)
    order_copy = pltpu.make_async_copy(order_v.at[pl.ds(0, 1)], order_s, order_sem)
    order_copy.start()

    order_copy.wait()
    lat_copy.wait()

    @pl.loop(0, blocks, unroll=8)
    def _(d):
        send[d] = lat[order_s[0, d]]

    received[me] = send[me]

    turn = 1 - 2 * c

    def send_blocks(some):
        for dz, dx, dy, dc in some:
            p = peer((turn * dz + nz, turn * dx + nx, turn * dy + ny, dc))
            pltpu.make_async_remote_copy(
                send.at[index_of(p)], received.at[me], send_sem, recv_sem, device_id=p, device_id_type=MESH
            ).start()

    pl.semaphore_wait(barrier, len(near))
    tell(in_x, rings[1])
    tell(in_y, rings[2])
    send_blocks(near)

    for copy in small:
        copy.wait()
    head_dim = query.shape[1]
    rank = lat.shape[2] // 2
    q0 = lax.dot_general(query[...], key_map[:, 0:head_dim], NT, preferred_element_type=F32)
    q1 = lax.dot_general(query[...], key_map[:, head_dim : 2 * head_dim], NT, preferred_element_type=F32)
    scale = LOG2E / float(head_dim) ** 0.5
    q_parts = jnp.concatenate(split3(jnp.concatenate([q0[0:8], q1[8:16]], 0) * scale), 0)
    length = length_s[batch_id]
    start = quads * (blocks * tokens)
    chunk_blocks = 16
    width = chunk_blocks * tokens
    best = jnp.full((16, 128), -1e30, F32)
    for i in range(blocks // chunk_blocks):
        keys = lat[i * chunk_blocks : (i + 1) * chunk_blocks, :, 0:rank].reshape(width, rank)
        s3 = lax.dot_general(q_parts, keys, NT, preferred_element_type=F32)
        s = s3[0:16] + s3[16:32] + s3[32:48]
        position = start + i * width + lax.broadcasted_iota(jnp.int32, (16, width), 1)
        s = jnp.where(position < length, s, -1e30)
        scores[:, i * width : (i + 1) * width] = s
        for j in range(width // 128):
            best = jnp.maximum(best, s[:, j * 128 : (j + 1) * 128])
    top = jnp.max(best, axis=1, keepdims=True)
    total = jnp.zeros((16, 128), F32)
    acc = jnp.zeros((32, rank), F32)
    for i in range(blocks // chunk_blocks):
        s = scores[:, i * width : (i + 1) * width]
        position = start + i * width + lax.broadcasted_iota(jnp.int32, (16, width), 1)
        w = jnp.where(position < length, jnp.exp2(s - top), 0.0)
        for j in range(width // 128):
            total = total + w[:, j * 128 : (j + 1) * 128]
        hi = w.astype(BF16)
        low = (w - hi.astype(F32)).astype(BF16)
        vals = lat[i * chunk_blocks : (i + 1) * chunk_blocks, :, rank : 2 * rank].reshape(width, rank)
        acc = acc + lax.dot_general(jnp.concatenate([hi, low], 0), vals, NN, preferred_element_type=F32)
    part_own[0:16] = acc[0:16] + acc[16:32]
    sums = jnp.sum(total, axis=1, keepdims=True)
    part_own[16:32] = jnp.where(lax.broadcasted_iota(jnp.int32, (16, 128), 1) < 64, top, sums)
    part_all[quads] = part_own[...]

    pl.semaphore_wait(in_x, nx - 1)
    pl.semaphore_wait(in_y, ny - 1)
    tell(in_all, rings[1])

    for k in range(1, 4):
        other_y = y + (k // 2) * (1 - 2 * (y % 2))
        other_c = (c + k % 2) % 2
        pltpu.make_async_remote_copy(
            part_own, part_all.at[quads], part_send, part_recv, device_id=(z, x, other_y, other_c), device_id_type=MESH
        ).start()

    send_blocks(planes)

    pl.semaphore_wait(in_all, nx - 1)

    three = part_all.at[pl.ds(0, 3)]
    pltpu.make_async_copy(three, three, part_recv).wait()
    tops = [part_all[k, 16:32, 0:1] for k in range(4)]
    top = jnp.maximum(jnp.maximum(tops[0], tops[1]), jnp.maximum(tops[2], tops[3]))
    total = jnp.zeros((16, 1), F32)
    acc = jnp.zeros((16, 128), F32)
    for k in range(4):
        factor = jnp.exp2(tops[k] - top)
        total = total + part_all[k, 16:32, 64:65] * factor
        acc = acc + part_all[k, 0:16] * factor
    mean = acc / total
    r0 = split_dot(mean[0:8], value_map[:, 0:head_dim], NN)
    r1 = split_dot(mean[8:16], value_map[:, head_dim : 2 * head_dim], NN)
    result[0:8] = r0
    result[8:16] = r1

    send_blocks(cube[:6])

    half = y // 2
    slot = half * (nx * nz) + x * nz + z
    dest_y = (y + c * (2 * (y % 2) - 1) + ny) % ny
    for dx, dz in random.Random(2).sample([(i, j) for i in range(nx) for j in range(nz)], nx * nz):
        pltpu.make_async_remote_copy(
            result, results.at[slot], res_send, res_recv,
            device_id=((z + dz) % nz, (x + dx) % nx, dest_y, 1 - c), device_id_type=MESH,
        ).start()

    send_blocks(cube[6:])

    per_half = nx * nz
    mine = c * half + (1 - c) * (1 - half)
    got = results.at[pl.ds(mine * per_half, per_half)]
    pltpu.make_async_copy(got, got, res_recv).wait()
    relay = pltpu.make_async_remote_copy(
        got, got, relay_send, relay_recv, device_id=(z, x, y, 1 - c), device_id_type=MESH
    )
    relay.start()
    relay.wait()
    for j in range(2):
        for zz in range(nz):
            for h in range(16):
                for xx in range(nx):
                    col = (zz * 16 + h) * 128
                    row = 2 * xx + j
                    attended[row : row + 1, col : col + 128] = results[j * per_half + xx * nz + zz, h : h + 1]

    pltpu.make_async_copy(part_all.at[pl.ds(0, 3)], part_all.at[pl.ds(0, 3)], part_send).wait()
    sixteen = results.at[pl.ds(0, per_half)]
    pltpu.make_async_copy(sixteen, sixteen, res_send).wait()
    rest = received.at[pl.ds(0, blocks - 1)]
    pltpu.make_async_copy(rest, rest, send_sem).wait()
    pltpu.make_async_copy(rest, rest, recv_sem).wait()


def store_kernel(received, attended, out0, out1, sem):
    copies = [
        pltpu.make_async_copy(received, out0, sem.at[0]),
        pltpu.make_async_copy(attended, out1, sem.at[1]),
    ]
    for copy in copies:
        copy.start()
    for copy in copies:
        copy.wait()


def body(latent, up_key, up_value, queries, lengths, block_dest):
    sizes = tuple(lax.axis_size(a) for a in AXES)
    groups, rank, width = up_key.shape
    blocks, tokens, both = latent.shape[1:]
    batch, heads, head_dim = queries.shape
    hbm = pl.BlockSpec(memory_space=pltpu.MemorySpace.HBM)
    vmem = pl.BlockSpec(memory_space=pltpu.MemorySpace.VMEM)
    dma = pltpu.SemaphoreType.DMA
    received, attended = pl.pallas_call(
        functools.partial(exchange_kernel, sizes),
        out_shape=(pltpu.VMEM((blocks, tokens, both), BF16), pltpu.VMEM((batch, heads * head_dim), F32)),
        in_specs=[hbm] * 6,
        out_specs=(vmem, vmem),
        scratch_shapes=[
            pltpu.VMEM((blocks, tokens, both), BF16),
            pltpu.VMEM((blocks, tokens, both), BF16),
            pltpu.VMEM((rank, width), BF16),
            pltpu.VMEM((rank, width), BF16),
            pltpu.VMEM((heads // groups, head_dim), BF16),
            pltpu.VMEM((1, blocks), jnp.int32),
            pltpu.VMEM((8, blocks), jnp.int32),
            pltpu.SMEM((1, blocks), jnp.int32),
            pltpu.SMEM((batch,), jnp.int32),
            pltpu.VMEM((16, blocks * tokens), F32),
            pltpu.VMEM((32, 128), F32),
            pltpu.VMEM((4, 32, 128), F32),
            pltpu.VMEM((16, 128), F32),
            pltpu.VMEM((groups * batch, 16, 128), F32),
            dma, dma((5,)), dma, dma, dma, dma, dma, dma, dma, dma, dma,
            pltpu.SemaphoreType.REGULAR, pltpu.SemaphoreType.REGULAR, pltpu.SemaphoreType.REGULAR,
        ],
        compiler_params=pltpu.CompilerParams(collective_id=1, has_side_effects=True),
        name="exchange",
    )(latent[0], up_key, up_value, queries, lengths, block_dest.reshape(-1, blocks))
    decode_latent, attended = pl.pallas_call(
        store_kernel,
        out_shape=(
            jax.ShapeDtypeStruct((blocks, tokens, both), BF16),
            jax.ShapeDtypeStruct((batch, heads * head_dim), F32),
        ),
        in_specs=[vmem, vmem],
        out_specs=(hbm, hbm),
        scratch_shapes=[dma((2,))],
        name="store",
    )(*[pltpu.with_memory_space_constraint(a, pltpu.MemorySpace.VMEM) for a in (received, attended)])
    return decode_latent.reshape(1, groups, blocks // groups, tokens, both), attended


def solution(mesh):
    finer = Mesh(mesh.devices.reshape(mesh.shape["grp"], 4, 4, 2), AXES)
    in_specs = (P("grp", SEQ, None, None), P(), P(), P(), P(), P())
    out_specs = (P(AXES, None, None, None, None), P())
    return jax.shard_map(body, mesh=finer, in_specs=in_specs, out_specs=out_specs, check_vma=False)
```

```python
import functools
import random

import jax
import jax.numpy as jnp
from jax import lax
from jax.experimental import pallas as pl
from jax.experimental.pallas import tpu as pltpu
from jax.sharding import Mesh
from jax.sharding import PartitionSpec as P

AXES = ("grp", "seq_0", "seq_1", "seq_2")
SEQ = AXES[1:]
MESH = pl.DeviceIdType.MESH
F32 = jnp.float32
BF16 = jnp.bfloat16
LOG2E = 1.4426950408889634
NT = (((1,), (1,)), ((), ()))
NN = (((1,), (0,)), ((), ()))
SEED = 3
EARLY = 36


def loads_of(flow):
    loads = []
    for steps in flow[:3]:
        loads += {0: [0, 0], 1: [1, 0], 2: [1, 1], 3: [0, 1]}[steps]
    return loads


def balanced(flows, total, seed):
    left = list(flows)
    random.Random(seed).shuffle(left)
    order = []
    while left:
        def uneven(flow):
            after = [a + b for a, b in zip(total, loads_of(flow))]
            mean = sum(after) / len(after)
            return sum((a - mean) ** 2 for a in after)

        best = min(left, key=uneven)
        left.remove(best)
        order.append(best)
        total[:] = [a + b for a, b in zip(total, loads_of(best))]
    return order


def flow_stages(sizes):
    nz, nx, ny, nc = sizes
    stages = [[], [], [], []]
    for dz in range(nz):
        for dx in range(nx):
            for dy in range(ny):
                for dc in range(nc):
                    stages[(dz > 0) + (dx > 0) + (dy > 0)].append((dz, dx, dy, dc))
    total = [0] * 6
    near = balanced(stages[0][1:] + stages[1], total, SEED)
    second = balanced(stages[2], total, SEED + 1)
    third = balanced(second[EARLY:] + stages[3], total, SEED + 2)
    return near, second[:EARLY], third


def split3(x):
    hi = x.astype(BF16)
    rest = x - hi.astype(F32)
    mid = rest.astype(BF16)
    low = (rest - mid.astype(F32)).astype(BF16)
    return hi, mid, low


def split_dot(x, w, dims):
    n = x.shape[0]
    out = lax.dot_general(jnp.concatenate(split3(x), 0), w, dims, preferred_element_type=F32)
    return out[0:n] + out[n : 2 * n] + out[2 * n : 3 * n]


def exchange_kernel(
    sizes,
    latent, up_key, up_value, queries, lengths, block_dest,
    received, attended,
    lat, send, key_map, value_map, query, dest_row, order_v, order_s, length_s,
    scores, part_own, part_all, result, results,
    lat_sem, small_sem, order_sem, send_sem, recv_sem, part_send, part_recv,
    res_send, res_recv, relay_send, relay_recv, in_x, in_y, in_all,
):
    nz, nx, ny, nc = sizes
    z, x, y, c = [lax.axis_index(a) for a in AXES]
    shard = (x * ny + y) * nc + c
    me = z * (nx * ny * nc) + shard
    blocks, tokens = lat.shape[0], lat.shape[1]
    quads = shard % 4
    batch_id = shard // 4

    def peer(offset):
        dz, dx, dy, dc = offset
        return ((z + dz) % nz, (x + dx) % nx, (y + dy) % ny, (c + dc) % nc)

    def index_of(p):
        return ((p[0] * nx + p[1]) * ny + p[2]) * nc + p[3]

    near, planes, cube = flow_stages(sizes)
    rings = [[(dz, 0, 0, 0) for dz in range(1, nz)], [(0, dx, 0, 0) for dx in range(1, nx)], [(0, 0, dy, 0) for dy in range(1, ny)]]
    barrier = pltpu.get_barrier_semaphore()

    def tell(semaphore, offsets):
        for offset in offsets:
            pl.semaphore_signal(semaphore, 1, device_id=peer(offset), device_id_type=MESH)


    dest_copy = pltpu.make_async_copy(block_dest.at[pl.ds(shard, 1)], dest_row, small_sem.at[0])
    dest_copy.start()
    lat_copy = pltpu.make_async_copy(latent, lat, lat_sem)
    piece = blocks // 8
    for k in range(8):
        part = pl.ds(k * piece, piece)
        pltpu.make_async_copy(latent.at[part], lat.at[part], lat_sem).start()
    small = [
        pltpu.make_async_copy(up_key.at[z], key_map, small_sem.at[1]),
        pltpu.make_async_copy(up_value.at[z], value_map, small_sem.at[2]),
        pltpu.make_async_copy(queries.at[batch_id, pl.ds(pl.multiple_of(z * 16, 16), 16)], query, small_sem.at[3]),
        pltpu.make_async_copy(lengths, length_s, small_sem.at[4]),
    ]
    for copy in small:
        copy.start()

    tell(barrier, near)

    dest_copy.wait()
    rows = lax.broadcasted_iota(jnp.int32, (blocks, blocks), 0)
    hot = jnp.where(rows == dest_row[...], 1.0, 0.0).astype(BF16)
    lanes = lax.broadcasted_iota(jnp.int32, (16, blocks), 1).astype(F32).astype(BF16)
    order = lax.dot_general(lanes, hot, NT, preferred_element_type=F32)[0:8].astype(jnp.int32)
    order_v[...] = jnp.clip(order, 0, blocks - 1)
    order_copy = pltpu.make_async_copy(order_v.at[pl.ds(0, 1)], order_s, order_sem)
    order_copy.start()

    order_copy.wait()
    lat_copy.wait()

    @pl.loop(0, blocks, unroll=8)
    def _(d):
        send[d] = lat[order_s[0, d]]

    received[me] = send[me]

    turn = 1 - 2 * c

    def send_blocks(some):
        for dz, dx, dy, dc in some:
            p = peer((turn * dz + nz, turn * dx + nx, turn * dy + ny, dc))
            pltpu.make_async_remote_copy(
                send.at[index_of(p)], received.at[me], send_sem, recv_sem, device_id=p, device_id_type=MESH
            ).start()

    pl.semaphore_wait(barrier, len(near))
    tell(in_x, rings[1])
    tell(in_y, rings[2])
    send_blocks(near)

    for copy in small:
        copy.wait()
    head_dim = query.shape[1]
    rank = lat.shape[2] // 2
    q0 = lax.dot_general(query[...], key_map[:, 0:head_dim], NT, preferred_element_type=F32)
    q1 = lax.dot_general(query[...], key_map[:, head_dim : 2 * head_dim], NT, preferred_element_type=F32)
    scale = LOG2E / float(head_dim) ** 0.5
    q_parts = jnp.concatenate(split3(jnp.concatenate([q0[0:8], q1[8:16]], 0) * scale), 0)
    length = length_s[batch_id]
    start = quads * (blocks * tokens)
    chunk_blocks = 16
    width = chunk_blocks * tokens
    best = jnp.full((16, 128), -1e30, F32)
    for i in range(blocks // chunk_blocks):
        keys = lat[i * chunk_blocks : (i + 1) * chunk_blocks, :, 0:rank].reshape(width, rank)
        s3 = lax.dot_general(q_parts, keys, NT, preferred_element_type=F32)
        s = s3[0:16] + s3[16:32] + s3[32:48]
        position = start + i * width + lax.broadcasted_iota(jnp.int32, (16, width), 1)
        s = jnp.where(position < length, s, -1e30)
        scores[:, i * width : (i + 1) * width] = s
        for j in range(width // 128):
            best = jnp.maximum(best, s[:, j * 128 : (j + 1) * 128])
    top = jnp.max(best, axis=1, keepdims=True)
    total = jnp.zeros((16, 128), F32)
    acc = jnp.zeros((32, rank), F32)
    for i in range(blocks // chunk_blocks):
        s = scores[:, i * width : (i + 1) * width]
        position = start + i * width + lax.broadcasted_iota(jnp.int32, (16, width), 1)
        w = jnp.where(position < length, jnp.exp2(s - top), 0.0)
        for j in range(width // 128):
            total = total + w[:, j * 128 : (j + 1) * 128]
        hi = w.astype(BF16)
        low = (w - hi.astype(F32)).astype(BF16)
        vals = lat[i * chunk_blocks : (i + 1) * chunk_blocks, :, rank : 2 * rank].reshape(width, rank)
        acc = acc + lax.dot_general(jnp.concatenate([hi, low], 0), vals, NN, preferred_element_type=F32)
    part_own[0:16] = acc[0:16] + acc[16:32]
    part_own[16:32] = jnp.broadcast_to(top, (16, 128))
    part_own[32:48] = jnp.broadcast_to(jnp.sum(total, axis=1, keepdims=True), (16, 128))
    part_all[quads] = part_own[...]

    pl.semaphore_wait(in_x, nx - 1)
    pl.semaphore_wait(in_y, ny - 1)
    tell(in_all, rings[1])

    for k in range(1, 4):
        other_y = y + (k // 2) * (1 - 2 * (y % 2))
        other_c = (c + k % 2) % 2
        pltpu.make_async_remote_copy(
            part_own, part_all.at[quads], part_send, part_recv, device_id=(z, x, other_y, other_c), device_id_type=MESH
        ).start()

    send_blocks(planes)

    pl.semaphore_wait(in_all, nx - 1)

    three = part_all.at[pl.ds(0, 3)]
    pltpu.make_async_copy(three, three, part_recv).wait()
    tops = [part_all[k, 16:32] for k in range(4)]
    top = jnp.maximum(jnp.maximum(tops[0], tops[1]), jnp.maximum(tops[2], tops[3]))
    total = jnp.zeros((16, 128), F32)
    acc = jnp.zeros((16, 128), F32)
    for k in range(4):
        factor = jnp.exp2(tops[k] - top)
        total = total + part_all[k, 32:48] * factor
        acc = acc + part_all[k, 0:16] * factor
    mean = acc / total
    r0 = split_dot(mean[0:8], value_map[:, 0:head_dim], NN)
    r1 = split_dot(mean[8:16], value_map[:, head_dim : 2 * head_dim], NN)
    result[0:8] = r0
    result[8:16] = r1

    send_blocks(cube[:20])

    half = y // 2
    slot = half * (nx * nz) + x * nz + z
    dest_y = (y + c * (2 * (y % 2) - 1) + ny) % ny
    for dx, dz in random.Random(2).sample([(i, j) for i in range(nx) for j in range(nz)], nx * nz):
        pltpu.make_async_remote_copy(
            result, results.at[slot], res_send, res_recv,
            device_id=((z + dz) % nz, (x + dx) % nx, dest_y, 1 - c), device_id_type=MESH,
        ).start()

    send_blocks(cube[20:])

    per_half = nx * nz
    mine = c * half + (1 - c) * (1 - half)
    got = results.at[pl.ds(mine * per_half, per_half)]
    pltpu.make_async_copy(got, got, res_recv).wait()
    relay = pltpu.make_async_remote_copy(
        got, got, relay_send, relay_recv, device_id=(z, x, y, 1 - c), device_id_type=MESH
    )
    relay.start()
    relay.wait()
    for j in range(2):
        for zz in range(nz):
            for h in range(16):
                for xx in range(nx):
                    col = (zz * 16 + h) * 128
                    row = 2 * xx + j
                    attended[row : row + 1, col : col + 128] = results[j * per_half + xx * nz + zz, h : h + 1]

    pltpu.make_async_copy(part_all.at[pl.ds(0, 3)], part_all.at[pl.ds(0, 3)], part_send).wait()
    sixteen = results.at[pl.ds(0, per_half)]
    pltpu.make_async_copy(sixteen, sixteen, res_send).wait()
    rest = received.at[pl.ds(0, blocks - 1)]
    pltpu.make_async_copy(rest, rest, send_sem).wait()
    pltpu.make_async_copy(rest, rest, recv_sem).wait()


def store_kernel(received, attended, out0, out1, sem):
    copies = [
        pltpu.make_async_copy(received, out0, sem.at[0]),
        pltpu.make_async_copy(attended, out1, sem.at[1]),
    ]
    for copy in copies:
        copy.start()
    for copy in copies:
        copy.wait()


def body(latent, up_key, up_value, queries, lengths, block_dest):
    sizes = tuple(lax.axis_size(a) for a in AXES)
    groups, rank, width = up_key.shape
    blocks, tokens, both = latent.shape[1:]
    batch, heads, head_dim = queries.shape
    hbm = pl.BlockSpec(memory_space=pltpu.MemorySpace.HBM)
    vmem = pl.BlockSpec(memory_space=pltpu.MemorySpace.VMEM)
    dma = pltpu.SemaphoreType.DMA
    received, attended = pl.pallas_call(
        functools.partial(exchange_kernel, sizes),
        out_shape=(pltpu.VMEM((blocks, tokens, both), BF16), pltpu.VMEM((batch, heads * head_dim), F32)),
        in_specs=[hbm] * 6,
        out_specs=(vmem, vmem),
        scratch_shapes=[
            pltpu.VMEM((blocks, tokens, both), BF16),
            pltpu.VMEM((blocks, tokens, both), BF16),
            pltpu.VMEM((rank, width), BF16),
            pltpu.VMEM((rank, width), BF16),
            pltpu.VMEM((heads // groups, head_dim), BF16),
            pltpu.VMEM((1, blocks), jnp.int32),
            pltpu.VMEM((8, blocks), jnp.int32),
            pltpu.SMEM((1, blocks), jnp.int32),
            pltpu.SMEM((batch,), jnp.int32),
            pltpu.VMEM((16, blocks * tokens), F32),
            pltpu.VMEM((48, 128), F32),
            pltpu.VMEM((4, 48, 128), F32),
            pltpu.VMEM((16, 128), F32),
            pltpu.VMEM((groups * batch, 16, 128), F32),
            dma, dma((5,)), dma, dma, dma, dma, dma, dma, dma, dma, dma,
            pltpu.SemaphoreType.REGULAR, pltpu.SemaphoreType.REGULAR, pltpu.SemaphoreType.REGULAR,
        ],
        compiler_params=pltpu.CompilerParams(collective_id=1, has_side_effects=True),
        name="exchange",
    )(latent[0], up_key, up_value, queries, lengths, block_dest.reshape(-1, blocks))
    decode_latent, attended = pl.pallas_call(
        store_kernel,
        out_shape=(
            jax.ShapeDtypeStruct((blocks, tokens, both), BF16),
            jax.ShapeDtypeStruct((batch, heads * head_dim), F32),
        ),
        in_specs=[vmem, vmem],
        out_specs=(hbm, hbm),
        scratch_shapes=[dma((2,))],
        name="store",
    )(*[pltpu.with_memory_space_constraint(a, pltpu.MemorySpace.VMEM) for a in (received, attended)])
    return decode_latent.reshape(1, groups, blocks // groups, tokens, both), attended


def solution(mesh):
    finer = Mesh(mesh.devices.reshape(mesh.shape["grp"], 4, 4, 2), AXES)
    in_specs = (P("grp", SEQ, None, None), P(), P(), P(), P(), P())
    out_specs = (P(AXES, None, None, None, None), P())
    return jax.shard_map(body, mesh=finer, in_specs=in_specs, out_specs=out_specs, check_vma=False)
```
